32 devices in a mesh: owner: 8 (over z, y), rows: 4 (over x, core).
Axes of the slice: x: 2, y: 2, z: 4, core: 2. Of those that a mesh axis runs over, the one named last changes fastest.
Arguments:
- master_down: float32 [16, 6400, 4096], P('owner', None, 'rows'), may hold values from -0.109375 to 0.109375
- router_weight: float32 [4096, 16], P('rows', 'owner'), may hold values from -0.09375 to 0.09375
- router_gain: float32 [4096], P('rows'), may hold values from 0.25 to 1.75
Outputs:
- final_down: bfloat16 [16, 6400, 4096], P('owner', 'rows')
- scale_down: float32 [16, 6400], P('owner', 'rows')
- serve_router: bfloat16 [4096, 16], replicated
The draws below stay inside these ranges and needn't reach their ends.
All inputs are finite; a program needn't handle non-finite values. Where the reference program divides by a largest or mean magnitude, that divisor is 1e-20 or more.
Results may differ from the reference program's by a relative error of at most 0.001.
Values may be sent and summed in bfloat16 or wider, within the bound.
A program may use at most 192 MiB of HBM per device.

```python
import jax
import jax.numpy as jnp

EXPERTS = 16
D_MODEL = 4096
D_EXPERT = 6400


def with_spikes(entries, rng, source, target, blocks, factor):
    owner, partner = [(jnp.arange(entries.shape[position]) // (entries.shape[position] // blocks)).reshape([-1 if axis == position else 1 for axis in range(entries.ndim)]) for position in (source, target)]
    chosen = jax.random.permutation(rng, blocks)[partner]
    strong = (owner == chosen) | (owner == (partner + blocks // 2) % blocks)
    return jnp.where(strong, factor * entries, entries)


def level_of(key, dims, cuts, low, largest):
    def one(axis_at, shards_of):
        heights = jax.random.uniform(jax.random.fold_in(jax.random.fold_in(key, 6), axis_at), (shards_of,), jnp.float32, low / len(cuts), largest / len(cuts))
        return jnp.repeat(jnp.exp(heights), dims[axis_at] // shards_of).reshape((-1,) + (1,) * (len(dims) - axis_at - 1))

    level = one(*cuts[0])
    for cut in cuts[1:]:
        level = level * one(*cut)
    return level


def gaussian(own_key, extent, deviation, bound, shards=(), dtype=jnp.bfloat16):
    drawn = deviation * jax.random.normal(own_key, extent, jnp.float32)
    if shards:
        drawn = drawn * level_of(own_key, extent, shards, -0.22, 0.18)
    return jnp.clip(drawn, -bound, bound).astype(dtype)


def heavy_noise(rng, dims, spread, bound, split, heavy, held_as=jnp.bfloat16):
    entries = spread * jax.random.normal(rng, dims, jnp.float32)
    if split:
        entries = entries * level_of(rng, dims, split, -0.22, 0.18)
    return jnp.clip(with_spikes(entries, jax.random.fold_in(rng, 3), *heavy), -bound, bound).astype(held_as)


def setup_inputs(seed: int = 0) -> dict:
    key_list = jax.random.split(jax.random.key(seed), 4)
    return {
        "master_down": heavy_noise(key_list[0], (EXPERTS, D_EXPERT, D_MODEL), D_EXPERT ** -0.5, 0.109375, ((0, 8), (2, 4)), (2, 1, 4, 2.0), jnp.float32),
        "router_weight": gaussian(key_list[1], (D_MODEL, EXPERTS), D_MODEL ** -0.5, 0.09375, ((0, 4), (1, 8)), jnp.float32),
        "router_gain": jnp.clip(1.0 + 0.15 * jax.random.normal(key_list[2], (D_MODEL,), jnp.float32), 0.25, 1.75),
    }


def reference(master_down, router_weight, router_gain):
    scale_down = jnp.sum(jnp.abs(master_down), axis=2) / D_MODEL
    final_down = (master_down / jnp.expand_dims(scale_down, 2)).astype(jnp.bfloat16)
    serve_router = (router_weight * router_gain[:, None]).astype(jnp.bfloat16)
    return final_down, scale_down, serve_router
```

```python
import functools

import jax
import jax.numpy as jnp
from jax import lax
from jax.experimental import pallas as pl
from jax.experimental.pallas import tpu as pltpu
from jax.sharding import PartitionSpec as P

LANES = 128
SLOTS = 3


def rows_per_block(quota, n):
    fits = [r for r in range(16, quota + 1, 16) if quota % r == 0 and (n * r) % LANES == 0]
    small = [r for r in fits if r * n <= 1280 and r <= 160]
    return max(small) if small else (min(fits) if fits else quota)


def kernel(n, steps, first, per, x_ref, out_ref, scale_ref, fbuf, nbuf, acc, mine, peers,
           load_sem, send_sem, recv_sem, own_sem, sum_send, sum_recv):
    me = lax.axis_index("rows")
    rows, width = fbuf.shape[2], fbuf.shape[3]
    groups = width // LANES

    barrier = pltpu.get_barrier_semaphore()
    for d in range(1, n):
        pl.semaphore_signal(
            barrier, inc=1, device_id={"rows": lax.rem(me + d, n)},
            device_id_type=pl.DeviceIdType.MESH,
        )

    def load(t):
        slot = t % SLOTS
        return pltpu.make_async_copy(x_ref.at[t // per, :, t % per], fbuf.at[slot], load_sem.at[slot])

    def prefetch(lo, hi):
        for t in range(lo, min(lo + SLOTS - 1, hi)):
            load(t).start()

    def stream(lo, hi, body):
        def step(t, carry):
            @pl.when(t + SLOTS - 1 < hi)
            def _():
                load(t + SLOTS - 1).start()

            load(t).wait()
            body(t, t % SLOTS)
            return carry

        lax.fori_loop(lo, hi, step, 0)

    def add_up(t, slot):
        for j in range(n):
            part = jnp.abs(fbuf[slot, j, :, :LANES])
            for g in range(1, groups):
                part = part + jnp.abs(fbuf[slot, j, :, g * LANES:(g + 1) * LANES])
            acc[j * rows:(j + 1) * rows, :] = part
        mine[t] = jnp.sum(acc[...].T, axis=0, keepdims=True)

    def exchange(turn, lo, hi):
        return [
            pltpu.make_async_remote_copy(
                src_ref=mine.at[pl.ds(lo, hi - lo)],
                dst_ref=peers.at[d - 1, pl.ds(lo, hi - lo)],
                send_sem=sum_send.at[turn, d - 1],
                recv_sem=sum_recv.at[turn, d - 1],
                device_id={"rows": lax.rem(me + d, n)},
                device_id_type=pl.DeviceIdType.MESH,
            )
            for d in range(1, n)
        ]

    def block(t, d):
        there = lax.rem(me + d, n)
        return pltpu.make_async_remote_copy(
            src_ref=nbuf.at[t, there],
            dst_ref=out_ref.at[t // per, pl.ds(pl.multiple_of((t % per) * rows, rows), rows),
                               pl.ds(pl.multiple_of(me * width, width), width)],
            send_sem=send_sem.at[d - 1, t],
            recv_sem=recv_sem.at[d - 1, t],
            device_id={"rows": there},
            device_id_type=pl.DeviceIdType.MESH,
        )

    def own(t):
        return pltpu.make_async_copy(
            nbuf.at[t, me],
            out_ref.at[t // per, pl.ds(pl.multiple_of((t % per) * rows, rows), rows),
                       pl.ds(pl.multiple_of(me * width, width), width)],
            own_sem.at[t],
        )

    def send(t):
        for d in range(1, n):
            block(t, d).start()
        own(t).start()

    def narrow(t):
        total = mine[t]
        for d in range(1, n):
            total = total + peers[d - 1, t]
        scale = total / (n * width)
        scale_ref[t] = scale
        acc[...] = jnp.broadcast_to(1.0 / scale, (LANES, n * rows)).T

    def scale_and_send(lo):
        def body(t, slot):
            narrow(t)
            for j in range(n):
                inverse = acc[j * rows:(j + 1) * rows, :]
                for g in range(groups):
                    cut = slice(g * LANES, (g + 1) * LANES)
                    nbuf[t, j, :, cut] = (fbuf[slot, j, :, cut] * inverse).astype(jnp.bfloat16)

            @pl.when(t > lo)
            def _():
                send(t - 1)

        return body

    prefetch(0, first)
    stream(0, first, add_up)
    prefetch(0, first)
    pl.semaphore_wait(barrier, n - 1)
    sums = exchange(0, 0, first)
    for copy in sums:
        copy.start()
    for copy in sums:
        copy.wait()
    stream(0, first, scale_and_send(0))
    if first < steps:
        prefetch(first, steps)
        stream(first, steps, add_up)
        prefetch(first, steps)
        sums = exchange(1, first, steps)
        for copy in sums:
            copy.start()
        send(first - 1)
        for copy in sums:
            copy.wait()
        stream(first, steps, scale_and_send(first))
    send(steps - 1)

    def finish(t, carry):
        for d in range(1, n):
            block(t, d).wait()
        own(t).wait()
        return carry

    lax.fori_loop(0, steps, finish, 0)


def per_device(n, master_down, router_weight, router_gain):
    experts, height, width = master_down.shape
    quota = height // n
    rows = rows_per_block(quota, n)
    per = quota // rows
    steps = experts * per
    first = min(max(3, -(-steps // 8)), steps)
    cut = n * rows
    final_down, scales = pl.pallas_call(
        functools.partial(kernel, n, steps, first, per),
        out_shape=(
            jax.ShapeDtypeStruct((experts, quota, n * width), jnp.bfloat16),
            jax.ShapeDtypeStruct((steps, 1, cut), jnp.float32),
        ),
        in_specs=[pl.BlockSpec(memory_space=pl.ANY)],
        out_specs=(pl.BlockSpec(memory_space=pl.ANY), pl.BlockSpec(memory_space=pltpu.VMEM)),
        scratch_shapes=[
            pltpu.VMEM((SLOTS, n, rows, width), jnp.float32),
            pltpu.VMEM((steps, n, rows, width), jnp.bfloat16),
            pltpu.VMEM((cut, LANES), jnp.float32),
            pltpu.VMEM((steps, 1, cut), jnp.float32),
            pltpu.VMEM((n - 1, steps, 1, cut), jnp.float32),
            pltpu.SemaphoreType.DMA((SLOTS,)),
            pltpu.SemaphoreType.DMA((n - 1, steps)),
            pltpu.SemaphoreType.DMA((n - 1, steps)),
            pltpu.SemaphoreType.DMA((steps,)),
            pltpu.SemaphoreType.DMA((2, n - 1)),
            pltpu.SemaphoreType.DMA((2, n - 1)),
        ],
        compiler_params=pltpu.CompilerParams(
            collective_id=0, has_side_effects=True, vmem_limit_bytes=48 * 1024 * 1024,
        ),
    )(master_down.reshape(experts, n, per, rows, width))
    by_device = scales.reshape(experts, per, n, rows)
    scale_down = lax.dynamic_index_in_dim(by_device, lax.axis_index("rows"), axis=2, keepdims=False)
    scale_down = scale_down.reshape(experts, quota)

    part_router = (router_weight * router_gain[:, None]).astype(jnp.bfloat16)
    row_router = lax.all_gather(part_router, "rows", axis=0, tiled=True)
    serve_router = lax.all_gather(row_router, "owner", axis=1, tiled=True)
    return (final_down, scale_down, serve_router)


def solution(mesh):
    return jax.shard_map(
        functools.partial(per_device, mesh.shape["rows"]),
        mesh=mesh,
        in_specs=(P("owner", None, "rows"), P("rows", "owner"), P("rows")),
        out_specs=(P("owner", "rows", None), P("owner", "rows"), P()),
        check_vma=False,
    )
```

```python
import functools

import jax
import jax.numpy as jnp
from jax import lax
from jax.experimental import pallas as pl
from jax.experimental.pallas import tpu as pltpu
from jax.sharding import PartitionSpec as P

LANES = 128
SLOTS = 3


def rows_per_block(quota, n):
    fits = [r for r in range(16, quota + 1, 16) if quota % r == 0 and (n * r) % LANES == 0]
    small = [r for r in fits if r * n <= 1280 and r <= 160]
    return max(small) if small else (min(fits) if fits else quota)


def kernel(n, owners, steps, first, per, x_ref, weight_ref, gain_ref, out_ref, scale_ref, router_ref, fbuf, nbuf, acc, mine, peers,
           strip, load_sem, send_sem, recv_sem, own_sem, sum_send, sum_recv, strip_send, strip_recv,
           router_send, router_recv):
    me = lax.axis_index("rows")
    home = lax.axis_index("owner")
    rows, width = fbuf.shape[2], fbuf.shape[3]
    groups = width // LANES

    barrier = pltpu.get_barrier_semaphore()
    for d in range(1, n):
        pl.semaphore_signal(
            barrier, inc=1, device_id={"rows": lax.rem(me + d, n)},
            device_id_type=pl.DeviceIdType.MESH,
        )
    for d in range(1, owners):
        pl.semaphore_signal(
            barrier, inc=1, device_id={"owner": lax.rem(home + d, owners)},
            device_id_type=pl.DeviceIdType.MESH,
        )
    strip[me] = (weight_ref[...] * gain_ref[...]).astype(jnp.bfloat16)

    def row_strip(d):
        return pltpu.make_async_remote_copy(
            src_ref=strip.at[me],
            dst_ref=strip.at[me],
            send_sem=strip_send.at[d - 1],
            recv_sem=strip_recv.at[d - 1],
            device_id={"rows": lax.rem(me + d, n)},
            device_id_type=pl.DeviceIdType.MESH,
        )

    def owner_strips(d):
        return pltpu.make_async_remote_copy(
            src_ref=strip,
            dst_ref=router_ref.at[home],
            send_sem=router_send.at[d - 1],
            recv_sem=router_recv.at[d - 1],
            device_id={"owner": lax.rem(home + d, owners)},
            device_id_type=pl.DeviceIdType.MESH,
        )

    def load(t):
        slot = t % SLOTS
        return pltpu.make_async_copy(x_ref.at[t // per, :, t % per], fbuf.at[slot], load_sem.at[slot])

    def prefetch(lo, hi):
        for t in range(lo, min(lo + SLOTS - 1, hi)):
            load(t).start()

    def stream(lo, hi, body):
        def step(t, carry):
            @pl.when(t + SLOTS - 1 < hi)
            def _():
                load(t + SLOTS - 1).start()

            load(t).wait()
            body(t, t % SLOTS)
            return carry

        lax.fori_loop(lo, hi, step, 0)

    def add_up(t, slot):
        for j in range(n):
            part = jnp.abs(fbuf[slot, j, :, :LANES])
            for g in range(1, groups):
                part = part + jnp.abs(fbuf[slot, j, :, g * LANES:(g + 1) * LANES])
            acc[j * rows:(j + 1) * rows, :] = part
        mine[t] = jnp.sum(acc[...].T, axis=0, keepdims=True)

    def exchange(turn, lo, hi):
        return [
            pltpu.make_async_remote_copy(
                src_ref=mine.at[pl.ds(lo, hi - lo)],
                dst_ref=peers.at[d - 1, pl.ds(lo, hi - lo)],
                send_sem=sum_send.at[turn, d - 1],
                recv_sem=sum_recv.at[turn, d - 1],
                device_id={"rows": lax.rem(me + d, n)},
                device_id_type=pl.DeviceIdType.MESH,
            )
            for d in range(1, n)
        ]

    def block(t, d):
        there = lax.rem(me + d, n)
        return pltpu.make_async_remote_copy(
            src_ref=nbuf.at[t, there],
            dst_ref=out_ref.at[t // per, pl.ds(pl.multiple_of((t % per) * rows, rows), rows),
                               pl.ds(pl.multiple_of(me * width, width), width)],
            send_sem=send_sem.at[d - 1, t],
            recv_sem=recv_sem.at[d - 1, t],
            device_id={"rows": there},
            device_id_type=pl.DeviceIdType.MESH,
        )

    def own(t):
        return pltpu.make_async_copy(
            nbuf.at[t, me],
            out_ref.at[t // per, pl.ds(pl.multiple_of((t % per) * rows, rows), rows),
                       pl.ds(pl.multiple_of(me * width, width), width)],
            own_sem.at[t],
        )

    def send(t):
        for d in range(1, n):
            block(t, d).start()
        own(t).start()

    def narrow(t):
        total = mine[t]
        for d in range(1, n):
            total = total + peers[d - 1, t]
        scale = total / (n * width)
        scale_ref[pl.ds(t, 1), :] = scale
        acc[...] = jnp.broadcast_to(1.0 / scale, (LANES, n * rows)).T

    def scale_and_send(lo):
        def body(t, slot):
            narrow(t)
            for j in range(n):
                inverse = acc[j * rows:(j + 1) * rows, :]
                for g in range(groups):
                    cut = slice(g * LANES, (g + 1) * LANES)
                    nbuf[t, j, :, cut] = (fbuf[slot, j, :, cut] * inverse).astype(jnp.bfloat16)

            @pl.when(t > lo)
            def _():
                send(t - 1)

        return body

    prefetch(0, first)
    stream(0, first, add_up)
    prefetch(0, first)
    pl.semaphore_wait(barrier, n - 1 + owners - 1)
    sums = exchange(0, 0, first)
    for copy in sums:
        copy.start()
    for d in range(1, n):
        row_strip(d).start()
    for copy in sums:
        copy.wait()
    stream(0, first, scale_and_send(0))
    for d in range(1, n):
        row_strip(d).wait()
    for d in range(1, owners):
        owner_strips(d).start()
    router_ref[home] = strip[...]
    if first < steps:
        prefetch(first, steps)
        stream(first, steps, add_up)
        prefetch(first, steps)
        sums = exchange(1, first, steps)
        for copy in sums:
            copy.start()
        send(first - 1)
        for copy in sums:
            copy.wait()
        stream(first, steps, scale_and_send(first))
    send(steps - 1)

    def finish(t, carry):
        for d in range(1, n):
            block(t, d).wait()
        own(t).wait()
        return carry

    lax.fori_loop(0, steps, finish, 0)
    for d in range(1, owners):
        owner_strips(d).wait()


def per_device(n, owners, master_down, router_weight, router_gain):
    experts, height, width = master_down.shape
    quota = height // n
    rows = rows_per_block(quota, n)
    per = quota // rows
    steps = experts * per
    first = min(max(3, -(-steps // 8)), steps)
    cut = n * rows
    depth, mine = router_weight.shape
    final_down, scales, strips = pl.pallas_call(
        functools.partial(kernel, n, owners, steps, first, per),
        out_shape=(
            jax.ShapeDtypeStruct((experts, quota, n * width), jnp.bfloat16),
            jax.ShapeDtypeStruct((steps, cut), jnp.float32),
            jax.ShapeDtypeStruct((owners, n, mine, depth), jnp.bfloat16),
        ),
        in_specs=[
            pl.BlockSpec(memory_space=pl.ANY),
            pl.BlockSpec(memory_space=pltpu.VMEM),
            pl.BlockSpec(memory_space=pltpu.VMEM),
        ],
        out_specs=(
            pl.BlockSpec(memory_space=pl.ANY),
            pl.BlockSpec(memory_space=pltpu.VMEM),
            pl.BlockSpec(memory_space=pltpu.VMEM),
        ),
        scratch_shapes=[
            pltpu.VMEM((SLOTS, n, rows, width), jnp.float32),
            pltpu.VMEM((steps, n, rows, width), jnp.bfloat16),
            pltpu.VMEM((cut, LANES), jnp.float32),
            pltpu.VMEM((steps, 1, cut), jnp.float32),
            pltpu.VMEM((n - 1, steps, 1, cut), jnp.float32),
            pltpu.VMEM((n, mine, depth), jnp.bfloat16),
            pltpu.SemaphoreType.DMA((SLOTS,)),
            pltpu.SemaphoreType.DMA((n - 1, steps)),
            pltpu.SemaphoreType.DMA((n - 1, steps)),
            pltpu.SemaphoreType.DMA((steps,)),
            pltpu.SemaphoreType.DMA((2, n - 1)),
            pltpu.SemaphoreType.DMA((2, n - 1)),
            pltpu.SemaphoreType.DMA((n - 1,)),
            pltpu.SemaphoreType.DMA((n - 1,)),
            pltpu.SemaphoreType.DMA((owners - 1,)),
            pltpu.SemaphoreType.DMA((owners - 1,)),
        ],
        compiler_params=pltpu.CompilerParams(
            collective_id=0, has_side_effects=True, vmem_limit_bytes=48 * 1024 * 1024,
        ),
    )(master_down.reshape(experts, n, per, rows, width), router_weight.T, router_gain[None, :])
    by_device = scales.reshape(experts, per, n, rows)
    scale_down = lax.dynamic_index_in_dim(by_device, lax.axis_index("rows"), axis=2, keepdims=False)
    scale_down = scale_down.reshape(experts, quota)

    serve_router = strips.transpose(0, 2, 1, 3).reshape(owners * mine, n * depth).T
    return (final_down, scale_down, serve_router)


def solution(mesh):
    return jax.shard_map(
        functools.partial(per_device, mesh.shape["rows"], mesh.shape["owner"]),
        mesh=mesh,
        in_specs=(P("owner", None, "rows"), P("rows", "owner"), P("rows")),
        out_specs=(P("owner", "rows", None), P("owner", "rows"), P()),
        check_vma=False,
    )
```
